32 devices in a mesh: expert: 4 (over z), vocab: 2 (over x), batch: 4 (over y, core).
Axes of the slice: x: 2, y: 2, z: 4, core: 2. Of those that a mesh axis runs over, the one named last changes fastest.
Arguments:
- resid: bfloat16 [4, 64, 6144], P('batch', ('expert', 'vocab')), may hold values from -6 to 6
- moe_gain: float32 [6144], replicated, may hold values from 0.25 to 2.5
- final_gain: float32 [6144], replicated, may hold values from 0.5 to 1.5
- router: bfloat16 [6144, 4], replicated, may hold values from -0.078125 to 0.078125
- w_gate: bfloat16 [4, 6144, 8192], P('expert', None, ('vocab', 'batch')), may hold values from -0.078125 to 0.078125
- w_up: bfloat16 [4, 6144, 8192], P('expert', None, ('vocab', 'batch')), may hold values from -0.078125 to 0.078125
- w_down: bfloat16 [4, 8192, 6144], P('expert', ('vocab', 'batch')), may hold values from -0.0625 to 0.0625
- lm_head: bfloat16 [16384, 6144], P(('expert', 'vocab')), may hold values from -6 to 6
- expert_ids: int32 [4, 64, 2], P('batch', ('expert', 'vocab')), may hold values from 0 to 3, all different within a row; in each aligned block of 8 rows (0 to 7, 8 to 15, ..., all dimensions but the last counted through in order) at most 5 rows name the same one
- target_ids: int32 [4, 64], P('batch'), may hold values from 0 to 16383
- choice_len: int32 [4, 8], P('batch'), may hold values from 1 to 32, 64 in all within a row
- choice_question: int32 [4, 8], P('batch'), may hold values from 0 to 1, as said below
Outputs:
- token_logprob: float32 [4, 64], P('batch', ('expert', 'vocab'))
- choice_prob: float32 [4, 8], P('batch')
The draws below stay inside these ranges and needn't reach their ends.
Inputs may be any that keep to these rules, and one draw needn't show every extreme that they name: `expert_ids`: A token's 2 experts differ; the rows of one device name each expert at most 5 times. `choice_len`: each group's lengths sum to 64. `choice_question`: in each group every question number appears exactly four times.
All inputs are finite; a program needn't handle non-finite values.
Results may differ from the reference program's by a relative error of at most 0.019.
Values may be sent and summed in bfloat16 or wider, within the bound.
A program may use at most 128 MiB of HBM per device.

```python
import math
import jax
import jax.numpy as jnp
import numpy as np
from jax import lax

D = 6144
TOPK = 2
FF_WIN = 8192
VOC_WIN = 16384
TOK_DEV = 8
EXPERTS = 4
GROUP_TOK = 64
CHOICES = 8
MOSTLEN = 32
CAP = 5
N_EXPERT = 4
N_VOCAB = 2
N_BATCH = 4


def draw_resid(key, part):
    base_key = jax.random.fold_in(key, 707)
    values = jnp.clip(jax.random.normal(base_key, (N_BATCH * GROUP_TOK, D), jnp.float32), -6.0, 6.0)
    return values.reshape(N_BATCH, GROUP_TOK, D).astype(jnp.bfloat16)


def draw_lm_head(key, part):
    base_key = jax.random.fold_in(key, 101)
    scale = 3.0 / D ** 0.5
    table = jnp.clip(jax.random.normal(base_key, (VOC_WIN, D), jnp.float32), -6.0, 6.0) * scale
    return jnp.clip(table, -6.0, 6.0).astype(jnp.bfloat16)


def shuffled_row(row_key):
    return jax.random.permutation(row_key, CHOICES) // 4


def draw_choice_question(key, part):
    row_keys = jax.random.split(jax.random.fold_in(key, 404), N_BATCH)
    return jax.vmap(shuffled_row)(row_keys).astype(jnp.int32)


def plant(drawn, own_key, low, top_value):
    longest = drawn.shape.index(max(drawn.shape))
    spots = []
    for shift in (0, 1):
        where = [jax.random.randint(jax.random.fold_in(own_key, axis), (), 0, length) for axis, length in enumerate(drawn.shape)]
        where[longest] = (where[longest] + shift) % drawn.shape[longest]
        spots.append(tuple(where))
    return drawn.at[spots[0]].set(low).at[spots[1]].set(top_value)


def block_levels(own_key, dims, cuts, smallest, top_value):
    def one(dim, parts):
        heights = jax.random.uniform(jax.random.fold_in(jax.random.fold_in(own_key, 6), dim), (parts,), jnp.float32, smallest / len(cuts), top_value / len(cuts))
        return jnp.repeat(jnp.exp(heights), dims[dim] // parts).reshape((-1,) + (1,) * (len(dims) - dim - 1))

    level = one(*cuts[0])
    for cut in cuts[1:]:
        level = level * one(*cut)
    return level


def length_profile(amount, total, reach, slope):
    loads = [(1 << 20) // math.isqrt(grade ** slope) + 1 for grade in range(2, amount + 1)]
    surplus, given = total - reach - (amount - 1), [1] * (amount - 1)
    while surplus > 0:
        free = [i for i in range(amount - 1) if given[i] < reach]
        mass, left = sum([loads[i] for i in free]), surplus
        for i in free:
            extra = min(reach - given[i], max(1, left * loads[i] // mass), surplus)
            given[i] = given[i] + extra
            surplus = surplus - extra
    return np.array([reach] + given)


def ragged(key, count, total, bound, skew):
    if count == 2:
        one = jax.random.randint(key, (), max(1, total - bound), min(bound, total - 1) + 1)
        return jnp.stack([one, total - one])
    tallies = jnp.asarray(length_profile(count, total, bound, skew), jnp.int32)
    pairs = (count - 1) // 2
    donor, taker = tallies[1:1 + 2 * pairs:2], tallies[2:2 + 2 * pairs:2]
    margin = jnp.minimum(donor - 1, bound - taker)
    passed = jax.random.randint(jax.random.fold_in(key, 1), (pairs,), 0, 1 << 20) % (margin + 1)
    tallies = tallies.at[1:1 + 2 * pairs:2].set(donor - passed).at[2:2 + 2 * pairs:2].set(taker + passed)
    return tallies[jax.random.permutation(jax.random.fold_in(key, 2), count)]


def deal_out(key, own, number, rows, amount, top, reach, skew):
    sequence = jax.random.permutation(key, amount)
    crowded, ordinary = portions_of(amount, rows * top, reach, skew, True), portions_of(amount, rows * top, reach, skew, False)
    places = jnp.arange(amount)

    def named(sizes, rotation):
        used = int((sizes > 0).sum())
        fixed = max(1, used // 4)
        moved = fixed + (places - fixed + rotation * (used - fixed)) % max(1, amount - fixed)
        return jnp.zeros((amount,), jnp.int32).at[sequence[jnp.where(places < fixed, places, moved)]].set(jnp.asarray(sizes, jnp.int32))

    sizes = jnp.where(number % 4 == 0, named(crowded, number // 4), named(ordinary, number - number // 4 - 1))
    mixed = jax.random.permutation(jax.random.fold_in(own, 3), amount)
    source_of, sink = mixed[0:amount // 2 * 2:2], mixed[1:amount // 2 * 2:2]
    room = jnp.minimum(sizes[source_of] - 1, reach - sizes[sink]) // 2
    room = jnp.where((source_of == sequence[0]) | (sink == sequence[0]) | (sizes[sink] == 0), 0, jnp.maximum(room, 0))
    moved = jax.random.randint(jax.random.fold_in(own, 4), (amount // 2,), 0, 1 << 20) % (room + 1)
    sizes = sizes.at[source_of].add(-moved).at[sink].add(moved)
    items = jnp.searchsorted(jnp.cumsum(sizes), jnp.arange(rows * top), side="right").astype(jnp.int32)
    grid = items.reshape(top, rows).T
    grid = grid[jax.random.permutation(jax.random.fold_in(own, 1), rows)]
    rotation = jax.random.randint(jax.random.fold_in(own, 2), (rows, 1), 0, top)
    return jnp.take_along_axis(grid, (jnp.arange(top)[None, :] + rotation) % top, axis=1)


def portions_of(count, total, bound, lean, full):
    loads = [(1 << 20) // math.isqrt(standing ** lean) + 1 for standing in range(1, count + 1)]
    largest = bound if full else min(bound, max(-(-total // count), total * loads[0] // sum(loads)))
    least = 1 if total - largest >= count - 1 else 0
    holding, surplus = [largest] + [least] * (count - 1), total - largest - least * (count - 1)
    while surplus > 0:
        free = [i for i in range(1, count) if holding[i] < largest] or [i for i in range(1, count) if holding[i] < bound]
        mass, remaining = sum([loads[i] for i in free]), surplus
        for i in free:
            more = min(bound - holding[i], max(1, remaining * loads[i] // mass), surplus)
            holding[i] = holding[i] + more
            surplus = surplus - more
    return np.array(holding)


def noise(key, extent, spread, bound, cuts=(), held_as=jnp.bfloat16):
    values = jax.random.normal(key, extent, jnp.float32) * spread
    if len(cuts) > 0:
        values = block_levels(key, extent, cuts, -0.22, 0.18) * values
    return jnp.clip(values, min=-bound, max=bound).astype(held_as)


def setup_inputs(seed: int = 0) -> dict:
    splits = jax.random.split(jax.random.key(seed), 13)
    resid = draw_resid(jax.random.fold_in(splits[12], 71), 0)
    moe_gain = jnp.clip(jnp.exp(jax.random.uniform(splits[1], (D,), jnp.float32, math.log(0.25), math.log(2.5))), 0.25, 2.5)
    final_gain = jnp.clip(1.0 + 0.1 * jax.random.normal(splits[2], (D,), jnp.float32), 0.5, 1.5)
    router = noise(splits[3], (D, EXPERTS), D ** -0.5, 0.078125)
    w_gate = noise(splits[4], (EXPERTS, D, FF_WIN), D ** -0.5, 0.078125, ((0, 4), (2, 8)))
    w_up = noise(splits[5], (EXPERTS, D, FF_WIN), D ** -0.5, 0.078125, ((0, 4), (2, 8)))
    w_down = noise(splits[6], (EXPERTS, FF_WIN, D), FF_WIN ** -0.5, 0.0625, ((0, 4), (1, 8)))
    lm_head = draw_lm_head(jax.random.fold_in(splits[12], 71), 0)
    expert_ids_keys = jax.random.split(jax.random.fold_in(splits[8], 1), N_BATCH * GROUP_TOK // TOK_DEV)
    expert_ids_turns = jax.random.permutation(jax.random.fold_in(splits[8], 3), N_BATCH * GROUP_TOK // TOK_DEV)
    expert_ids = jax.vmap(lambda own, number: deal_out(jax.random.fold_in(splits[8], 2), own, number, TOK_DEV, EXPERTS, TOPK, CAP, 2))(expert_ids_keys, expert_ids_turns).reshape((N_BATCH, GROUP_TOK, TOPK))
    target_ids = plant(jax.random.randint(splits[9], (N_BATCH, GROUP_TOK), 0, VOC_WIN), jax.random.fold_in(splits[9], 1), 0, VOC_WIN - 1).astype(jnp.int32)
    choice_len = jax.vmap(lambda own: ragged(own, CHOICES, GROUP_TOK, MOSTLEN, 1))(jax.random.split(splits[10], N_BATCH)).reshape((N_BATCH, CHOICES)).astype(jnp.int32)
    choice_question = draw_choice_question(jax.random.fold_in(splits[12], 71), 0)
    return {"resid": resid, "moe_gain": moe_gain, "final_gain": final_gain, "router": router, "w_gate": w_gate, "w_up": w_up, "w_down": w_down, "lm_head": lm_head, "expert_ids": expert_ids, "target_ids": target_ids, "choice_len": choice_len, "choice_question": choice_question}


epsilon = 1e-05

def rms_scale(values, gain):
    mean_square = lax.optimization_barrier(jnp.mean(values * values, axis=-1, keepdims=True))
    return values * lax.rsqrt(mean_square + epsilon) * gain

def choice_member(lengths, positions):
    ends = jnp.cumsum(lengths, dtype=jnp.int32)
    starts = ends - lengths
    return (positions[None, :] >= starts[:, None]) & (positions[None, :] < ends[:, None])

def choice_softmax(choice_total, lengths, questions):
    average = choice_total / lengths.astype(jnp.float32)
    same_question = questions[:, None] == questions[None, :]
    question_top = lax.optimization_barrier(jnp.max(jnp.where(same_question, average[None, :], -jnp.inf), axis=1))
    raised = jnp.exp(average - question_top)
    denominator = lax.optimization_barrier(jnp.sum(jnp.where(same_question, raised[None, :], 0.0), axis=1))
    return raised / denominator

def reference(resid, moe_gain, final_gain, router, w_gate, w_up, w_down, lm_head, expert_ids, target_ids, choice_len, choice_question):
    groups, group_tokens, model_width = resid.shape
    stream = resid.reshape(-1, model_width).astype(jnp.float32)
    row_count = stream.shape[0]
    normed_in = rms_scale(stream, moe_gain).astype(jnp.bfloat16)
    router_logit = jnp.dot(normed_in, router, preferred_element_type=jnp.float32)
    route_ids = expert_ids.reshape(row_count, -1).astype(jnp.int32)
    picked = jnp.take_along_axis(router_logit, route_ids, axis=1)
    gate_weights = 1.0 / lax.optimization_barrier(jnp.sum(jnp.exp(picked[:, None, :] - picked[:, :, None]), axis=2))
    flat_ids = route_ids.reshape(-1)
    flat_gates = gate_weights.reshape(-1)
    token_of = jnp.arange(flat_ids.shape[0], dtype=jnp.int32) // route_ids.shape[1]
    slices = N_VOCAB * N_BATCH
    bound_rows = N_EXPERT * N_VOCAB * N_BATCH * CAP

    def one_expert(combined, expert):
        found = flat_ids == expert
        chosen_rows = jnp.nonzero(found, size=bound_rows, fill_value=0)[0].astype(jnp.int32)
        valid = jnp.arange(bound_rows, dtype=jnp.int32) < jnp.sum(found.astype(jnp.int32))
        tokens = token_of[chosen_rows]
        block_rows = normed_in[tokens]
        gate_part = jnp.dot(block_rows, w_gate[expert], preferred_element_type=jnp.float32)
        up_part = jnp.dot(block_rows, w_up[expert], preferred_element_type=jnp.float32)
        hidden = (jax.nn.silu(gate_part) * up_part).astype(jnp.bfloat16)
        hidden = hidden.reshape(bound_rows, slices, -1)
        down_parts = w_down[expert].reshape(slices, -1, model_width)

        def add_slice(running, slice_index):
            part = jnp.dot(hidden[:, slice_index], down_parts[slice_index], preferred_element_type=jnp.float32).astype(jnp.bfloat16)
            part = lax.optimization_barrier(part)
            return (running + part.astype(jnp.float32), None)
        running, _ = lax.scan(add_slice, jnp.zeros((bound_rows, model_width), jnp.float32), jnp.arange(slices, dtype=jnp.int32))
        expert_out = lax.optimization_barrier(running.astype(jnp.bfloat16)).astype(jnp.float32)
        weight = jnp.where(valid, flat_gates[chosen_rows], 0.0)
        return (combined.at[tokens].add(weight[:, None] * expert_out), None)
    combined, _ = lax.scan(one_expert, jnp.zeros((row_count, model_width), jnp.float32), jnp.arange(EXPERTS, dtype=jnp.int32))
    mixed_rows = stream + combined
    normed_out = rms_scale(mixed_rows, final_gain).astype(jnp.bfloat16)
    logits = lax.dot_general(normed_out, lm_head, (((1,), (1,)), ((), ())), preferred_element_type=jnp.float32)
    largest = lax.optimization_barrier(jnp.max(logits, axis=1))
    log_total = largest + jnp.log(lax.optimization_barrier(jnp.sum(jnp.exp(logits - largest[:, None]), axis=1)))
    target_logit = jnp.take_along_axis(logits, target_ids.reshape(-1, 1).astype(jnp.int32), axis=1)[:, 0]
    token_logprob = (target_logit - log_total).reshape(groups, group_tokens)
    positions = jnp.arange(group_tokens, dtype=jnp.int32)

    def group_probs(logprob_row, lengths, questions):
        member = choice_member(lengths, positions)
        choice_total = lax.optimization_barrier(jnp.sum(jnp.where(member, logprob_row[None, :], 0.0), axis=1))
        return choice_softmax(choice_total, lengths, questions)
    choice_prob = jax.vmap(group_probs)(token_logprob, choice_len, choice_question)
    return (token_logprob, choice_prob)
```

```python
import functools

import jax
import jax.numpy as jnp
from jax import lax
from jax.experimental import pallas as pl
from jax.experimental.pallas import tpu as pltpu
from jax.sharding import PartitionSpec as P

epsilon = 1e-05


def joined(array, axis, combine):
    everything = jax.tree.map(lambda part: lax.all_gather(part, axis), array)
    leading = jax.tree.map(lambda part: part[0], everything)

    def lap(k, so_far):
        return combine(so_far, jax.tree.map(lambda part: part[k], everything))

    return lax.fori_loop(1, lax.axis_size(axis), lap, leading)


def rms_scale(values, gain):
    mean_square = jnp.mean(values * values, axis=-1, keepdims=True)
    return values * lax.rsqrt(mean_square + epsilon) * gain


def route_gates(router_logit, route_ids):
    expert_count = router_logit.shape[1]
    matches = route_ids[:, :, None] == jnp.arange(expert_count, dtype=jnp.int32)[None, None, :]
    picked = jnp.sum(jnp.where(matches, router_logit[:, None, :], 0.0), axis=2)
    return 1.0 / jnp.sum(jnp.exp(picked[:, None, :] - picked[:, :, None]), axis=2)


def expand_rows(block_rows, gate_cols, up_cols):
    gate_part = jnp.dot(block_rows, gate_cols, preferred_element_type=jnp.float32)
    up_part = jnp.dot(block_rows, up_cols, preferred_element_type=jnp.float32)
    return (jax.nn.silu(gate_part) * up_part).astype(jnp.bfloat16)


def choice_member(lengths, positions):
    ends = jnp.cumsum(lengths, dtype=jnp.int32)
    starts = ends - lengths
    return (positions[None, :] >= starts[:, None]) & (positions[None, :] < ends[:, None])


def choice_softmax(choice_total, lengths, questions):
    average = choice_total / lengths.astype(jnp.float32)
    same_question = questions[:, None] == questions[None, :]
    question_top = jnp.max(jnp.where(same_question, average[None, :], -jnp.inf), axis=1)
    raised = jnp.exp(average - question_top)
    denominator = jnp.sum(jnp.where(same_question, raised[None, :], 0.0), axis=1)
    return raised / denominator


def merge_stats(first, second):
    top_value = jnp.maximum(first[0], second[0])
    summed = first[1] * jnp.exp(first[0] - top_value) + second[1] * jnp.exp(second[0] - top_value)
    return (top_value, summed, first[2] + second[2])


def on_device(
    resid,
    moe_gain,
    final_gain,
    router,
    w_gate,
    w_up,
    w_down,
    lm_head,
    expert_ids,
    target_ids,
    choice_len,
    choice_question,
):
    stream = resid[0].astype(jnp.float32)
    token_count, model_width = stream.shape
    normed_in = rms_scale(stream, moe_gain).astype(jnp.bfloat16)
    router_logit = jnp.dot(normed_in, router, preferred_element_type=jnp.float32)
    route_ids = expert_ids[0]
    route_count = route_ids.shape[1]
    gate_weights = route_gates(router_logit, route_ids)
    expert_count = lax.axis_size("expert")
    bucket_size = max(2, (token_count * route_count + expert_count - 1) // expert_count + 1)
    flat_ids = route_ids.reshape(-1)
    expert_match = (flat_ids[:, None] == jnp.arange(expert_count, dtype=jnp.int32)[None, :]).astype(
        jnp.int32
    )
    earlier = jnp.cumsum(expert_match, axis=0, dtype=jnp.int32) - expert_match
    slot_index = flat_ids * bucket_size + jnp.sum(earlier * expert_match, axis=1)
    slot_match = (
        slot_index[:, None] == jnp.arange(expert_count * bucket_size, dtype=jnp.int32)[None, :]
    ).astype(jnp.float32)
    slot_match = slot_match.reshape(token_count, route_count, -1)
    dispatch = jnp.sum(slot_match, axis=1).astype(jnp.bfloat16)
    combine_weights = jnp.sum(slot_match * gate_weights[:, :, None], axis=1)
    buckets = lax.dot_general(
        dispatch, normed_in, (((0,), (0,)), ((), ())), preferred_element_type=jnp.float32
    )
    buckets = buckets.astype(jnp.bfloat16).reshape(expert_count, bucket_size, model_width)
    gate_cols = w_gate[0]
    up_cols = w_up[0]
    down_rows = w_down[0]
    arrived = lax.all_to_all(buckets, "expert", split_axis=0, concat_axis=0, tiled=True).reshape(
        -1, model_width
    )
    hidden = expand_rows(
        lax.all_gather(arrived, ("vocab", "batch"), axis=0, tiled=True), gate_cols, up_cols
    )
    expert_sum = lax.psum_scatter(
        jnp.dot(hidden, down_rows, preferred_element_type=jnp.float32).astype(jnp.bfloat16),
        ("vocab", "batch"),
        scatter_dimension=0,
        tiled=True,
    )
    outgoing = expert_sum.reshape(expert_count, bucket_size, model_width)
    returned = lax.all_to_all(outgoing, "expert", split_axis=0, concat_axis=0, tiled=True)
    returned_rows = returned.reshape(-1, model_width).astype(jnp.float32)
    mixed_rows = stream + jnp.dot(combine_weights, returned_rows, precision=lax.Precision.HIGHEST)
    normed_out = rms_scale(mixed_rows, final_gain).astype(jnp.bfloat16)
    head_index = lax.axis_index(("expert", "vocab"))
    vocab_share = lm_head.shape[0]
    vocab_ids = jnp.arange(vocab_share, dtype=jnp.int32) + head_index * vocab_share
    targets = target_ids[0]
    group_tokens = targets.shape[0]
    logits = lax.dot_general(
        lax.all_gather(normed_out, ("expert", "vocab"), axis=0, tiled=True),
        lm_head,
        (((1,), (1,)), ((), ())),
        preferred_element_type=jnp.float32,
    )
    block_top = jnp.max(logits, axis=1)
    block_sum = jnp.sum(jnp.exp(logits - block_top[:, None]), axis=1)
    block_hit = jnp.sum(jnp.where(targets[:, None] == vocab_ids[None, :], logits, 0.0), axis=1)
    fresh = (block_top, block_sum, block_hit)
    largest, spread_sum, chosen = tuple((fresh[slot] for slot in range(3)))
    lengths = choice_len[0]
    questions = choice_question[0]
    own_first = head_index * token_count
    group_positions = jnp.arange(group_tokens, dtype=jnp.int32)
    best, summed, target_sum = joined(
        (largest, spread_sum, chosen), ("expert", "vocab"), merge_stats
    )
    group_logprob = target_sum - (best + jnp.log(summed))
    choice_total = jnp.sum(
        jnp.where(choice_member(lengths, group_positions), group_logprob[None, :], 0.0), axis=1
    )
    own_logprob = lax.dynamic_slice_in_dim(group_logprob, own_first, token_count, 0)
    choice_prob = choice_softmax(choice_total, lengths, questions)
    return (own_logprob.reshape(1, -1), choice_prob.reshape(1, -1))


MESH = pl.DeviceIdType.MESH
VMEM_BYTES = 67043328
COLUMN_CHUNKS = 4


def greet(partners):
    barrier = pltpu.get_barrier_semaphore()
    for partner in partners:
        pl.semaphore_signal(barrier, inc=1, device_id=partner, device_id_type=MESH)
    pl.semaphore_wait(barrier, len(partners))


def push(src, dst, send_sem, recv_sem, partner):
    return pltpu.make_async_remote_copy(
        src_ref=src,
        dst_ref=dst,
        send_sem=send_sem,
        recv_sem=recv_sem,
        device_id=partner,
        device_id_type=MESH,
    )


def experts_kernel(
    ne,
    nv,
    nb,
    own_ref,
    resid_ref,
    gates_ref,
    gain_ref,
    wg_hbm,
    wu_hbm,
    wd_hbm,
    out_ref,
    wg,
    wu,
    wd,
    zin,
    xs,
    hid,
    part,
    rpair,
    rchip,
    zs,
    zo,
    w_sem,
    z_send,
    z_recv,
    c_send,
    c_recv,
    p_send,
    p_recv,
    rp_send,
    rp_recv,
    rc_send,
    rc_recv,
    rz_send,
    rz_recv,
):
    e, v, b = lax.axis_index("expert"), lax.axis_index("vocab"), lax.axis_index("batch")
    half = nb // 2
    chips = nv * half
    core = lax.rem(b, 2)
    other = 1 - core
    chip = v * half + b // 2
    tokens, width = own_ref.shape
    block = ne * tokens

    def at_expert(k):
        return (lax.rem(e + k, ne), v, b)

    def at_chip(k):
        c = lax.rem(chip + k, chips)
        return (e, c // half, lax.rem(c, half) * 2 + core)

    mate = (e, v, b + 1 - 2 * core)

    loads = [
        pltpu.make_async_copy(src, dst, w_sem.at[i])
        for i, (src, dst) in enumerate(((wg_hbm.at[0], wg), (wu_hbm.at[0], wu), (wd_hbm.at[0], wd)))
    ]
    for load in loads:
        load.start()
    greet(
        [at_expert(k) for k in range(1, ne)] + [at_chip(k) for k in range(1, chips)] + [mate]
    )

    z_copies = [
        push(own_ref, zin.at[e], z_send.at[k], z_recv.at[k], at_expert(k)) for k in range(1, ne)
    ]
    for copy in z_copies:
        copy.start()
    zin[e] = own_ref[...]
    for copy in z_copies:
        copy.wait_recv()
    xs[core, chip] = (
        zin[...].astype(jnp.float32).reshape(block, width).astype(jnp.bfloat16)
    )

    c_copies = [
        push(
            xs.at[core, chip], xs.at[core, chip], c_send.at[k], c_recv.at[k], at_chip(k)
        )
        for k in range(1, chips)
    ]
    p_copies = []
    for k in range(chips):
        c = lax.rem(chip + chips - k, chips)
        p_copies.append(push(xs.at[core, c], xs.at[core, c], p_send.at[k], p_recv.at[k], mate))
    for copy in c_copies:
        copy.start()
    p_copies[0].start()
    for k in range(1, chips):
        c_copies[k - 1].wait_recv()
        p_copies[k].start()
    for copy in p_copies:
        copy.wait_recv()

    rows = 2 * chips * block
    loads[0].wait()
    loads[1].wait()
    hidden_width = wg.shape[1]
    tile = min(256, hidden_width)

    @pl.loop(0, hidden_width // tile)
    def _(i):
        cols = pl.ds(pl.multiple_of(i * tile, tile), tile)
        x = xs[...].reshape(rows, width)
        g = jnp.dot(x, wg[:, cols], preferred_element_type=jnp.float32)
        u = jnp.dot(x, wu[:, cols], preferred_element_type=jnp.float32)
        hid[:, cols] = (g / (1.0 + jnp.exp(-g)) * u).astype(jnp.bfloat16)

    loads[2].wait()
    chunk = width // COLUMN_CHUNKS
    down_tile = 512 if chunk % 512 == 0 else 128
    rp, rc, rz = [], [], []

    def columns(j):
        return pl.ds(j * chunk, chunk)

    def down(j):
        @pl.loop(0, chunk // down_tile)
        def _(i):
            cols = pl.ds(pl.multiple_of(j * chunk + i * down_tile, down_tile), down_tile)
            y = jnp.dot(hid[...], wd[:, cols], preferred_element_type=jnp.float32)
            part[:, :, :, cols] = y.astype(jnp.bfloat16).reshape(2, chips, block, down_tile)

        copy = push(
            part.at[other, :, :, columns(j)],
            rpair.at[:, :, columns(j)],
            rp_send.at[j],
            rp_recv.at[j],
            mate,
        )
        copy.start()
        rp.append(copy)

    def pair_sum(j):
        rp[j].wait_recv()
        total = part[core, :, :, columns(j)].astype(jnp.float32) + rpair[
            :, :, columns(j)
        ].astype(jnp.float32)
        part[core, :, :, columns(j)] = total.astype(jnp.bfloat16)
        for k in range(1, chips):
            to = lax.rem(chip + k, chips)
            copy = push(
                part.at[core, to, :, columns(j)],
                rchip.at[k - 1, :, columns(j)],
                rc_send.at[j, k],
                rc_recv.at[j, k],
                at_chip(k),
            )
            copy.start()
            rc.append(copy)

    def plane_sum(j):
        for k in range(1, chips):
            rc[j * (chips - 1) + k - 1].wait_recv()
        total = part[core, chip, :, columns(j)].astype(jnp.float32)
        for k in range(1, chips):
            total = total + rchip[k - 1, :, columns(j)].astype(jnp.float32)
        zs[:, :, columns(j)] = total.reshape(ne, tokens, chunk).astype(jnp.bfloat16)
        for k in range(1, ne):
            to = lax.rem(e + k, ne)
            copy = push(
                zs.at[to, :, columns(j)],
                zo.at[e, :, columns(j)],
                rz_send.at[j, k],
                rz_recv.at[j, k],
                at_expert(k),
            )
            copy.start()
            rz.append(copy)
        zo[e, :, columns(j)] = zs[e, :, columns(j)]

    for j in range(COLUMN_CHUNKS):
        down(j)
        if j >= 1:
            pair_sum(j - 1)
    pair_sum(COLUMN_CHUNKS - 1)
    for j in range(COLUMN_CHUNKS):
        plane_sum(j)
    for copy in rz:
        copy.wait_recv()
    gates = gates_ref[...]
    mixed = resid_ref[...].astype(jnp.float32)
    for k in range(ne):
        mixed = mixed + gates[:, k : k + 1] * zo[k].astype(jnp.float32)
    scale = lax.rsqrt(jnp.mean(mixed * mixed, axis=-1, keepdims=True) + epsilon)
    out_ref[...] = (mixed * scale * gain_ref[...]).astype(jnp.bfloat16)
    for copy in z_copies + c_copies + p_copies + rp + rc + rz:
        copy.wait_send()


def experts_call(sizes, own, resid, gates, gain, w_gate, w_up, w_down):
    ne, nv, nb = sizes
    tokens, width = own.shape
    hidden_width = w_gate.shape[2]
    chips = nv * nb // 2
    block = ne * tokens
    bf16 = jnp.bfloat16
    dma = pltpu.SemaphoreType.DMA
    vm = pl.BlockSpec(memory_space=pltpu.VMEM)
    anywhere = pl.BlockSpec(memory_space=pl.ANY)
    n = COLUMN_CHUNKS
    return pl.pallas_call(
        functools.partial(experts_kernel, ne, nv, nb),
        out_shape=jax.ShapeDtypeStruct((tokens, width), bf16),
        in_specs=[vm, vm, vm, vm, anywhere, anywhere, anywhere],
        out_specs=vm,
        scratch_shapes=[
            pltpu.VMEM((width, hidden_width), bf16),
            pltpu.VMEM((width, hidden_width), bf16),
            pltpu.VMEM((hidden_width, width), bf16),
            pltpu.VMEM((ne, tokens, width), bf16),
            pltpu.VMEM((2, chips, block, width), bf16),
            pltpu.VMEM((2 * chips * block, hidden_width), bf16),
            pltpu.VMEM((2, chips, block, width), bf16),
            pltpu.VMEM((chips, block, width), bf16),
            pltpu.VMEM((max(1, chips - 1), block, width), bf16),
            pltpu.VMEM((ne, tokens, width), bf16),
            pltpu.VMEM((ne, tokens, width), bf16),
            dma((3,)),
            dma((ne,)),
            dma((ne,)),
            dma((chips,)),
            dma((chips,)),
            dma((chips,)),
            dma((chips,)),
            dma((n,)),
            dma((n,)),
            dma((n, chips)),
            dma((n, chips)),
            dma((n, ne)),
            dma((n, ne)),
        ],
        compiler_params=pltpu.CompilerParams(
            collective_id=0, has_side_effects=True, vmem_limit_bytes=VMEM_BYTES - 2 * 1024 * 1024
        ),
        name="experts",
    )(own, resid, gates, gain, w_gate, w_up, w_down)


def head_kernel(
    ne, nv, own_ref, target_ref, head_hbm, out_ref, head, ys, stats, h_sem, y_send, y_recv, s_send, s_recv
):
    e, v, b = lax.axis_index("expert"), lax.axis_index("vocab"), lax.axis_index("batch")
    peers = ne * nv
    me = e * nv + v
    share, width = head.shape
    tokens = own_ref.shape[0]
    rows = peers * tokens
    lanes = out_ref.shape[1]
    tile = min(256, share)

    def at(k):
        p = lax.rem(me + k, peers)
        return (p // nv, lax.rem(p, nv), b)

    parts = h_sem.shape[0]
    depth = share // parts
    loads = [
        pltpu.make_async_copy(
            head_hbm.at[pl.ds(i * depth, depth)], head.at[pl.ds(i * depth, depth)], h_sem.at[i]
        )
        for i in range(parts)
    ]
    for load in loads:
        load.start()
    greet([at(k) for k in range(1, peers)])
    copies = [
        push(own_ref, ys.at[me], y_send.at[k], y_recv.at[k], at(k)) for k in range(1, peers)
    ]
    for copy in copies:
        copy.start()
    ys[me] = own_ref[...]
    for copy in copies:
        copy.wait_recv()
    for load in loads:
        load.wait()
    y = ys[...].astype(jnp.float32).reshape(rows, width).astype(jnp.bfloat16)
    targets = target_ref[...]

    def lap(i, carry):
        top, total, hit = carry
        first = pl.multiple_of(i * tile, tile)
        logits = lax.dot_general(
            y,
            head[pl.ds(first, tile), :],
            (((1,), (1,)), ((), ())),
            preferred_element_type=jnp.float32,
        )
        ids = lax.broadcasted_iota(jnp.int32, logits.shape, 1) + (me * share + first)
        new_top = jnp.maximum(top, jnp.max(logits, axis=1, keepdims=True))
        total = total * jnp.exp(top - new_top) + jnp.sum(
            jnp.exp(logits - new_top), axis=1, keepdims=True
        )
        hit = hit + jnp.sum(jnp.where(ids == targets, logits, 0.0), axis=1, keepdims=True)
        return new_top, total, hit

    zero = jnp.zeros((rows, 1), jnp.float32)
    top, total, hit = lax.fori_loop(
        0, share // tile, lap, (jnp.full((rows, 1), -jnp.inf, jnp.float32), zero, zero)
    )
    eye = lax.broadcasted_iota(jnp.int32, (rows, lanes), 0) == lax.broadcasted_iota(
        jnp.int32, (rows, lanes), 1
    )

    def laid(column):
        return jnp.sum(jnp.where(eye, column, 0.0), axis=0, keepdims=True)

    line = lax.broadcasted_iota(jnp.int32, (8, lanes), 0)
    stats[me] = jnp.where(
        line == 0, laid(top), jnp.where(line == 1, laid(total), jnp.where(line == 2, laid(hit), 0.0))
    )
    sends = [
        push(stats.at[me], stats.at[me], s_send.at[k], s_recv.at[k], at(k)) for k in range(1, peers)
    ]
    for copy in sends:
        copy.start()
    for copy in sends:
        copy.wait_recv()
    every = stats[...]
    best = jnp.max(every[:, 0:1, :], axis=0)
    summed = jnp.sum(every[:, 1:2, :] * jnp.exp(every[:, 0:1, :] - best[None]), axis=0)
    chosen = jnp.sum(every[:, 2:3, :], axis=0)
    used = lax.broadcasted_iota(jnp.int32, (1, lanes), 1) < rows
    logprob = chosen - (best + jnp.log(jnp.where(used, summed, 1.0)))
    out_ref[...] = jnp.broadcast_to(logprob, out_ref.shape)
    for copy in copies + sends:
        copy.wait_send()


def head_call(sizes, own, targets, lm_head):
    ne, nv, nb = sizes
    tokens, width = own.shape
    peers = ne * nv
    dma = pltpu.SemaphoreType.DMA
    vm = pl.BlockSpec(memory_space=pltpu.VMEM)
    return pl.pallas_call(
        functools.partial(head_kernel, ne, nv),
        out_shape=jax.ShapeDtypeStruct((8, 128), jnp.float32),
        in_specs=[vm, vm, pl.BlockSpec(memory_space=pl.ANY)],
        out_specs=vm,
        scratch_shapes=[
            pltpu.VMEM(lm_head.shape, jnp.bfloat16),
            pltpu.VMEM((peers, tokens, width), jnp.bfloat16),
            pltpu.VMEM((peers, 8, 128), jnp.float32),
            dma((4,)),
            dma((peers,)),
            dma((peers,)),
            dma((peers,)),
            dma((peers,)),
        ],
        compiler_params=pltpu.CompilerParams(
            collective_id=1, has_side_effects=True, vmem_limit_bytes=VMEM_BYTES - 2 * 1024 * 1024
        ),
        name="head",
    )(own, targets, lm_head)


def kernels_fit(sizes, resid, w_gate, lm_head):
    ne, nv, nb = sizes
    tokens, width = resid.shape[1:]
    hidden_width = w_gate.shape[2]
    rows = ne * nv * nb * tokens
    need = 2 * (3 * width * hidden_width + rows * (3 * width + hidden_width) + 8 * ne * tokens * width)
    group = ne * nv * tokens
    head_need = 2 * (lm_head.shape[0] * width + 4 * group * width)
    return (
        nb % 2 == 0
        and tokens % 8 == 0
        and width % (128 * COLUMN_CHUNKS) == 0
        and hidden_width % 256 == 0
        and lm_head.shape[0] % 256 == 0
        and group <= 128
        and max(need, head_need) < VMEM_BYTES - 4 * 1024 * 1024
    )


def on_device_kernels(
    sizes,
    resid,
    moe_gain,
    final_gain,
    router,
    w_gate,
    w_up,
    w_down,
    lm_head,
    expert_ids,
    target_ids,
    choice_len,
    choice_question,
):
    ne, nv, nb = sizes
    stream = resid[0].astype(jnp.float32)
    token_count = stream.shape[0]
    normed_in = rms_scale(stream, moe_gain).astype(jnp.bfloat16)
    router_logit = jnp.dot(normed_in, router, preferred_element_type=jnp.float32)
    route_ids = expert_ids[0]
    gate_weights = route_gates(router_logit, route_ids)
    gates = jnp.sum(
        jnp.where(
            route_ids[:, :, None] == jnp.arange(ne, dtype=jnp.int32)[None, None, :],
            gate_weights[:, :, None],
            0.0,
        ),
        axis=1,
    )
    normed_out = experts_call(
        sizes, normed_in, resid[0], gates, final_gain.reshape(1, -1), w_gate, w_up, w_down
    )
    targets = target_ids[0]
    group_tokens = targets.shape[0]
    found = head_call(sizes, normed_out, targets.reshape(-1, 1), lm_head)
    group_logprob = found[0, :group_tokens]
    lengths = choice_len[0]
    positions = jnp.arange(group_tokens, dtype=jnp.int32)
    choice_total = jnp.sum(
        jnp.where(choice_member(lengths, positions), group_logprob[None, :], 0.0), axis=1
    )
    own_first = lax.axis_index(("expert", "vocab")) * token_count
    own_logprob = lax.dynamic_slice_in_dim(group_logprob, own_first, token_count, 0)
    choice_prob = choice_softmax(choice_total, lengths, choice_question[0])
    return (own_logprob.reshape(1, -1), choice_prob.reshape(1, -1))


def either(sizes, *arrays):
    if kernels_fit(sizes, arrays[0], arrays[4], arrays[7]):
        return on_device_kernels(sizes, *arrays)
    return on_device(*arrays)


def solution(mesh):
    sizes = tuple(mesh.shape[axis] for axis in ("expert", "vocab", "batch"))
    return jax.shard_map(
        functools.partial(either, sizes),
        mesh=mesh,
        in_specs=(
            P("batch", ("expert", "vocab"), None),
            P(),
            P(),
            P(),
            P("expert", None, ("vocab", "batch")),
            P("expert", None, ("vocab", "batch")),
            P("expert", ("vocab", "batch"), None),
            P(("expert", "vocab"), None),
            P("batch", ("expert", "vocab"), None),
            P("batch", None),
            P("batch", None),
            P("batch", None),
        ),
        out_specs=(P("batch", ("expert", "vocab")), P("batch", None)),
        check_vma=False,
    )
```

```python
import functools

import jax
import jax.numpy as jnp
from jax import lax
from jax.experimental import pallas as pl
from jax.experimental.pallas import tpu as pltpu
from jax.sharding import PartitionSpec as P

epsilon = 1e-05


def joined(array, axis, combine):
    everything = jax.tree.map(lambda part: lax.all_gather(part, axis), array)
    leading = jax.tree.map(lambda part: part[0], everything)

    def lap(k, so_far):
        return combine(so_far, jax.tree.map(lambda part: part[k], everything))

    return lax.fori_loop(1, lax.axis_size(axis), lap, leading)


def rms_scale(values, gain):
    mean_square = jnp.mean(values * values, axis=-1, keepdims=True)
    return values * lax.rsqrt(mean_square + epsilon) * gain


def route_gates(router_logit, route_ids):
    expert_count = router_logit.shape[1]
    matches = route_ids[:, :, None] == jnp.arange(expert_count, dtype=jnp.int32)[None, None, :]
    picked = jnp.sum(jnp.where(matches, router_logit[:, None, :], 0.0), axis=2)
    return 1.0 / jnp.sum(jnp.exp(picked[:, None, :] - picked[:, :, None]), axis=2)


def expand_rows(block_rows, gate_cols, up_cols):
    gate_part = jnp.dot(block_rows, gate_cols, preferred_element_type=jnp.float32)
    up_part = jnp.dot(block_rows, up_cols, preferred_element_type=jnp.float32)
    return (jax.nn.silu(gate_part) * up_part).astype(jnp.bfloat16)


def choice_member(lengths, positions):
    ends = jnp.cumsum(lengths, dtype=jnp.int32)
    starts = ends - lengths
    return (positions[None, :] >= starts[:, None]) & (positions[None, :] < ends[:, None])


def choice_softmax(choice_total, lengths, questions):
    average = choice_total / lengths.astype(jnp.float32)
    same_question = questions[:, None] == questions[None, :]
    question_top = jnp.max(jnp.where(same_question, average[None, :], -jnp.inf), axis=1)
    raised = jnp.exp(average - question_top)
    denominator = jnp.sum(jnp.where(same_question, raised[None, :], 0.0), axis=1)
    return raised / denominator


def merge_stats(first, second):
    top_value = jnp.maximum(first[0], second[0])
    summed = first[1] * jnp.exp(first[0] - top_value) + second[1] * jnp.exp(second[0] - top_value)
    return (top_value, summed, first[2] + second[2])


def on_device(
    resid,
    moe_gain,
    final_gain,
    router,
    w_gate,
    w_up,
    w_down,
    lm_head,
    expert_ids,
    target_ids,
    choice_len,
    choice_question,
):
    stream = resid[0].astype(jnp.float32)
    token_count, model_width = stream.shape
    normed_in = rms_scale(stream, moe_gain).astype(jnp.bfloat16)
    router_logit = jnp.dot(normed_in, router, preferred_element_type=jnp.float32)
    route_ids = expert_ids[0]
    route_count = route_ids.shape[1]
    gate_weights = route_gates(router_logit, route_ids)
    expert_count = lax.axis_size("expert")
    bucket_size = max(2, (token_count * route_count + expert_count - 1) // expert_count + 1)
    flat_ids = route_ids.reshape(-1)
    expert_match = (flat_ids[:, None] == jnp.arange(expert_count, dtype=jnp.int32)[None, :]).astype(
        jnp.int32
    )
    earlier = jnp.cumsum(expert_match, axis=0, dtype=jnp.int32) - expert_match
    slot_index = flat_ids * bucket_size + jnp.sum(earlier * expert_match, axis=1)
    slot_match = (
        slot_index[:, None] == jnp.arange(expert_count * bucket_size, dtype=jnp.int32)[None, :]
    ).astype(jnp.float32)
    slot_match = slot_match.reshape(token_count, route_count, -1)
    dispatch = jnp.sum(slot_match, axis=1).astype(jnp.bfloat16)
    combine_weights = jnp.sum(slot_match * gate_weights[:, :, None], axis=1)
    buckets = lax.dot_general(
        dispatch, normed_in, (((0,), (0,)), ((), ())), preferred_element_type=jnp.float32
    )
    buckets = buckets.astype(jnp.bfloat16).reshape(expert_count, bucket_size, model_width)
    gate_cols = w_gate[0]
    up_cols = w_up[0]
    down_rows = w_down[0]
    arrived = lax.all_to_all(buckets, "expert", split_axis=0, concat_axis=0, tiled=True).reshape(
        -1, model_width
    )
    hidden = expand_rows(
        lax.all_gather(arrived, ("vocab", "batch"), axis=0, tiled=True), gate_cols, up_cols
    )
    expert_sum = lax.psum_scatter(
        jnp.dot(hidden, down_rows, preferred_element_type=jnp.float32).astype(jnp.bfloat16),
        ("vocab", "batch"),
        scatter_dimension=0,
        tiled=True,
    )
    outgoing = expert_sum.reshape(expert_count, bucket_size, model_width)
    returned = lax.all_to_all(outgoing, "expert", split_axis=0, concat_axis=0, tiled=True)
    returned_rows = returned.reshape(-1, model_width).astype(jnp.float32)
    mixed_rows = stream + jnp.dot(combine_weights, returned_rows, precision=lax.Precision.HIGHEST)
    normed_out = rms_scale(mixed_rows, final_gain).astype(jnp.bfloat16)
    head_index = lax.axis_index(("expert", "vocab"))
    vocab_share = lm_head.shape[0]
    vocab_ids = jnp.arange(vocab_share, dtype=jnp.int32) + head_index * vocab_share
    targets = target_ids[0]
    group_tokens = targets.shape[0]
    logits = lax.dot_general(
        lax.all_gather(normed_out, ("expert", "vocab"), axis=0, tiled=True),
        lm_head,
        (((1,), (1,)), ((), ())),
        preferred_element_type=jnp.float32,
    )
    block_top = jnp.max(logits, axis=1)
    block_sum = jnp.sum(jnp.exp(logits - block_top[:, None]), axis=1)
    block_hit = jnp.sum(jnp.where(targets[:, None] == vocab_ids[None, :], logits, 0.0), axis=1)
    fresh = (block_top, block_sum, block_hit)
    largest, spread_sum, chosen = tuple((fresh[slot] for slot in range(3)))
    lengths = choice_len[0]
    questions = choice_question[0]
    own_first = head_index * token_count
    group_positions = jnp.arange(group_tokens, dtype=jnp.int32)
    best, summed, target_sum = joined(
        (largest, spread_sum, chosen), ("expert", "vocab"), merge_stats
    )
    group_logprob = target_sum - (best + jnp.log(summed))
    choice_total = jnp.sum(
        jnp.where(choice_member(lengths, group_positions), group_logprob[None, :], 0.0), axis=1
    )
    own_logprob = lax.dynamic_slice_in_dim(group_logprob, own_first, token_count, 0)
    choice_prob = choice_softmax(choice_total, lengths, questions)
    return (own_logprob.reshape(1, -1), choice_prob.reshape(1, -1))


MESH = pl.DeviceIdType.MESH
VMEM_BYTES = 67043328
COLUMN_CHUNKS = 4


def greet(partners):
    barrier = pltpu.get_barrier_semaphore()
    for partner in partners:
        pl.semaphore_signal(barrier, inc=1, device_id=partner, device_id_type=MESH)
    pl.semaphore_wait(barrier, len(partners))


def push(src, dst, send_sem, recv_sem, partner):
    return pltpu.make_async_remote_copy(
        src_ref=src,
        dst_ref=dst,
        send_sem=send_sem,
        recv_sem=recv_sem,
        device_id=partner,
        device_id_type=MESH,
    )


def experts_kernel(
    ne,
    nv,
    nb,
    own_ref,
    resid_ref,
    gates_ref,
    gain_ref,
    wg_hbm,
    wu_hbm,
    wd_hbm,
    out_ref,
    wg,
    wu,
    wd,
    zin,
    xs,
    hid,
    part,
    rpair,
    rchip,
    zs,
    zo,
    w_sem,
    z_send,
    z_recv,
    c_send,
    c_recv,
    p_send,
    p_recv,
    rp_send,
    rp_recv,
    rc_send,
    rc_recv,
    rz_send,
    rz_recv,
):
    e, v, b = lax.axis_index("expert"), lax.axis_index("vocab"), lax.axis_index("batch")
    core = lax.rem(b, 2)
    other = 1 - core
    tokens, width = own_ref.shape
    block = ne * tokens
    chips = 4
    across = (e, 1 - v, b)
    along = (e, v, lax.rem(b + 2, 4))
    mate = (e, v, b + 1 - 2 * core)
    near = {1: along, 2: across}

    def at_expert(k):
        return (lax.rem(e + k, ne), v, b)

    loads = [
        pltpu.make_async_copy(src, dst, w_sem.at[i])
        for i, (src, dst) in enumerate(((wg_hbm.at[0], wg), (wu_hbm.at[0], wu), (wd_hbm.at[0], wd)))
    ]
    for load in loads:
        load.start()
    greet([at_expert(k) for k in range(1, ne)] + [across, along, mate])

    z_copies = [
        push(own_ref, zin.at[e], z_send.at[k], z_recv.at[k], at_expert(k)) for k in range(1, ne)
    ]
    for copy in z_copies:
        copy.start()
    zin[e] = own_ref[...]
    for copy in z_copies:
        copy.wait_recv()
    xs[0, core] = zin[...].astype(jnp.float32).reshape(block, width).astype(jnp.bfloat16)

    part_width = width // 2

    def piece(h):
        return pl.ds(h * part_width, part_width)

    def plane_push(src_slot, dst_slot, h, n):
        return push(
            xs.at[src_slot, core, :, piece(h)],
            xs.at[dst_slot, core, :, piece(h)],
            c_send.at[dst_slot, h],
            c_recv.at[dst_slot, h],
            near[n],
        )

    def mate_push(slot, h):
        return push(
            xs.at[slot, core, :, piece(h)],
            xs.at[slot, core, :, piece(h)],
            p_send.at[slot, h],
            p_recv.at[slot, h],
            mate,
        )

    c_copies = {(n, h): plane_push(0, n, h, n) for n in (1, 2) for h in (0, 1)}
    c_copies[3, 0] = plane_push(2, 3, 0, 1)
    c_copies[3, 1] = plane_push(1, 3, 1, 2)
    p_copies = {(slot, h): mate_push(slot, h) for slot in range(4) for h in (0, 1)}
    for key in ((2, 0), (1, 1), (2, 1), (1, 0)):
        c_copies[key].start()
    p_copies[0, 0].start()
    p_copies[0, 1].start()
    for key, follow in (((2, 0), (3, 0)), ((1, 1), (3, 1)), ((1, 0), None), ((2, 1), None)):
        c_copies[key].wait_recv()
        if follow is not None:
            c_copies[follow].start()
        p_copies[key].start()
    hidden_width = wg.shape[1]
    tile = min(256, hidden_width)
    rows = 2 * block

    def expand(first, count):
        @pl.loop(0, hidden_width // tile)
        def _(i):
            cols = pl.ds(pl.multiple_of(i * tile, tile), tile)
            x = xs[first : first + count].reshape(count * rows, width)
            g = jnp.dot(x, wg[:, cols], preferred_element_type=jnp.float32)
            u = jnp.dot(x, wu[:, cols], preferred_element_type=jnp.float32)
            hid[first * rows : (first + count) * rows, cols] = (
                g / (1.0 + jnp.exp(-g)) * u
            ).astype(jnp.bfloat16)

    loads[0].wait()
    loads[1].wait()
    for slot in (0, 1):
        for h in (0, 1):
            p_copies[slot, h].wait_recv()
    expand(0, 2)
    for h in (0, 1):
        c_copies[3, h].wait_recv()
        p_copies[3, h].start()
    for slot in (2, 3):
        for h in (0, 1):
            p_copies[slot, h].wait_recv()
    expand(2, 2)

    loads[2].wait()
    chunk = width // COLUMN_CHUNKS
    down_tile = 512 if chunk % 512 == 0 else 128
    rp, rd, rn, rz = {}, {}, {}, {}

    def columns(j):
        return pl.ds(j * chunk, chunk)

    def wide(ref_value):
        return ref_value.astype(jnp.float32)

    def down(j):
        @pl.loop(0, chunk // down_tile)
        def _(i):
            cols = pl.ds(pl.multiple_of(j * chunk + i * down_tile, down_tile), down_tile)
            y = jnp.dot(hid[...], wd[:, cols], preferred_element_type=jnp.float32)
            part[:, :, :, cols] = y.astype(jnp.bfloat16).reshape(chips, 2, block, down_tile)

        rp[j] = push(
            part.at[:, other, :, columns(j)],
            rpair.at[:, :, columns(j)],
            rp_send.at[j],
            rp_recv.at[j],
            mate,
        )
        rp[j].start()

    def neighbour_push(slot, j):
        return push(
            part.at[slot, core, :, columns(j)],
            rchip.at[slot - 1, :, columns(j)],
            rc_send.at[j, slot],
            rc_recv.at[j, slot],
            near[slot],
        )

    def pair_sum(j):
        rp[j].wait_recv()
        total = wide(part[:, core, :, columns(j)]) + wide(rpair[:, :, columns(j)])
        part[:, core, :, columns(j)] = total.astype(jnp.bfloat16)
        via = 2 - j % 2
        rd[j] = push(
            part.at[3, core, :, columns(j)],
            rchip.at[2, :, columns(j)],
            rc_send.at[j, 3],
            rc_recv.at[j, 3],
            near[via],
        )
        rd[j].start()
        rn[j, via] = neighbour_push(via, j)
        rn[j, via].start()

    def relay(j):
        last = 1 + j % 2
        rd[j].wait_recv()
        total = wide(part[last, core, :, columns(j)]) + wide(rchip[2, :, columns(j)])
        part[last, core, :, columns(j)] = total.astype(jnp.bfloat16)
        rn[j, last] = neighbour_push(last, j)
        rn[j, last].start()

    def plane_sum(j):
        rn[j, 1].wait_recv()
        rn[j, 2].wait_recv()
        total = wide(part[0, core, :, columns(j)])
        total = total + wide(rchip[0, :, columns(j)]) + wide(rchip[1, :, columns(j)])
        zs[:, :, columns(j)] = total.reshape(ne, tokens, chunk).astype(jnp.bfloat16)
        for k in range(1, ne):
            to = lax.rem(e + k, ne)
            rz[j, k] = push(
                zs.at[to, :, columns(j)],
                zo.at[e, :, columns(j)],
                rz_send.at[j, k],
                rz_recv.at[j, k],
                at_expert(k),
            )
            rz[j, k].start()
        zo[e, :, columns(j)] = zs[e, :, columns(j)]

    for j in range(COLUMN_CHUNKS):
        down(j)
        if j >= 1:
            pair_sum(j - 1)
    pair_sum(COLUMN_CHUNKS - 1)
    for j in range(COLUMN_CHUNKS):
        relay(j)
        if j >= 1:
            plane_sum(j - 1)
    plane_sum(COLUMN_CHUNKS - 1)
    for copy in rz.values():
        copy.wait_recv()
    gates = gates_ref[...]
    mixed = resid_ref[...].astype(jnp.float32)
    for k in range(ne):
        mixed = mixed + gates[:, k : k + 1] * zo[k].astype(jnp.float32)
    scale = lax.rsqrt(jnp.mean(mixed * mixed, axis=-1, keepdims=True) + epsilon)
    out_ref[...] = (mixed * scale * gain_ref[...]).astype(jnp.bfloat16)
    for group in (c_copies, p_copies, rp, rd, rn, rz):
        for copy in group.values():
            copy.wait_send()
    for copy in z_copies:
        copy.wait_send()


def experts_call(sizes, own, resid, gates, gain, w_gate, w_up, w_down):
    ne, nv, nb = sizes
    tokens, width = own.shape
    hidden_width = w_gate.shape[2]
    chips = nv * nb // 2
    block = ne * tokens
    bf16 = jnp.bfloat16
    dma = pltpu.SemaphoreType.DMA
    vm = pl.BlockSpec(memory_space=pltpu.VMEM)
    anywhere = pl.BlockSpec(memory_space=pl.ANY)
    n = COLUMN_CHUNKS
    return pl.pallas_call(
        functools.partial(experts_kernel, ne, nv, nb),
        out_shape=jax.ShapeDtypeStruct((tokens, width), bf16),
        in_specs=[vm, vm, vm, vm, anywhere, anywhere, anywhere],
        out_specs=vm,
        scratch_shapes=[
            pltpu.VMEM((width, hidden_width), bf16),
            pltpu.VMEM((width, hidden_width), bf16),
            pltpu.VMEM((hidden_width, width), bf16),
            pltpu.VMEM((ne, tokens, width), bf16),
            pltpu.VMEM((chips, 2, block, width), bf16),
            pltpu.VMEM((2 * chips * block, hidden_width), bf16),
            pltpu.VMEM((chips, 2, block, width), bf16),
            pltpu.VMEM((chips, block, width), bf16),
            pltpu.VMEM((max(1, chips - 1), block, width), bf16),
            pltpu.VMEM((ne, tokens, width), bf16),
            pltpu.VMEM((ne, tokens, width), bf16),
            dma((3,)),
            dma((ne,)),
            dma((ne,)),
            dma((chips, 2)),
            dma((chips, 2)),
            dma((chips, 2)),
            dma((chips, 2)),
            dma((n,)),
            dma((n,)),
            dma((n, chips)),
            dma((n, chips)),
            dma((n, ne)),
            dma((n, ne)),
        ],
        compiler_params=pltpu.CompilerParams(
            collective_id=0, has_side_effects=True, vmem_limit_bytes=VMEM_BYTES - 2 * 1024 * 1024
        ),
        name="experts",
    )(own, resid, gates, gain, w_gate, w_up, w_down)


def head_kernel(
    ne, nv, own_ref, target_ref, head_hbm, out_ref, head, ys, stats, h_sem, y_send, y_recv, s_send, s_recv
):
    e, v, b = lax.axis_index("expert"), lax.axis_index("vocab"), lax.axis_index("batch")
    peers = ne * nv
    me = e * nv + v
    share, width = head.shape
    tokens = own_ref.shape[0]
    rows = peers * tokens
    lanes = out_ref.shape[1]
    tile = min(256, share)

    def at(k):
        p = lax.rem(me + k, peers)
        return (p // nv, lax.rem(p, nv), b)

    parts = h_sem.shape[0]
    depth = share // parts
    loads = [
        pltpu.make_async_copy(
            head_hbm.at[pl.ds(i * depth, depth)], head.at[pl.ds(i * depth, depth)], h_sem.at[i]
        )
        for i in range(parts)
    ]
    for load in loads:
        load.start()
    greet([at(k) for k in range(1, peers)])
    across = (e, 1 - v, b)
    along = [
        push(own_ref, ys.at[me], y_send.at[0, k], y_recv.at[0, k], (lax.rem(e + k, ne), v, b))
        for k in range(1, ne)
    ]
    turns = [push(own_ref, ys.at[me], y_send.at[1, 0], y_recv.at[1, 0], across)]
    for k in range(1, ne):
        slot = lax.rem(e + ne - k, ne) * nv + v
        turns.append(push(ys.at[slot], ys.at[slot], y_send.at[1, k], y_recv.at[1, k], across))
    for copy in along:
        copy.start()
    turns[0].start()
    ys[me] = own_ref[...]
    for k in [1] + [k for k in range(ne - 1, 1, -1)]:
        along[k - 1].wait_recv()
        turns[k].start()
    for copy in turns:
        copy.wait_recv()
    copies = along + turns
    for load in loads:
        load.wait()
    y = ys[...].astype(jnp.float32).reshape(rows, width).astype(jnp.bfloat16)
    targets = target_ref[...]

    def lap(i, carry):
        top, total, hit = carry
        first = pl.multiple_of(i * tile, tile)
        logits = lax.dot_general(
            y,
            head[pl.ds(first, tile), :],
            (((1,), (1,)), ((), ())),
            preferred_element_type=jnp.float32,
        )
        ids = lax.broadcasted_iota(jnp.int32, logits.shape, 1) + (me * share + first)
        new_top = jnp.maximum(top, jnp.max(logits, axis=1, keepdims=True))
        total = total * jnp.exp(top - new_top) + jnp.sum(
            jnp.exp(logits - new_top), axis=1, keepdims=True
        )
        hit = hit + jnp.sum(jnp.where(ids == targets, logits, 0.0), axis=1, keepdims=True)
        return new_top, total, hit

    zero = jnp.zeros((rows, 1), jnp.float32)
    top, total, hit = lax.fori_loop(
        0, share // tile, lap, (jnp.full((rows, 1), -jnp.inf, jnp.float32), zero, zero)
    )
    eye = lax.broadcasted_iota(jnp.int32, (rows, lanes), 0) == lax.broadcasted_iota(
        jnp.int32, (rows, lanes), 1
    )

    def laid(column):
        return jnp.sum(jnp.where(eye, column, 0.0), axis=0, keepdims=True)

    line = lax.broadcasted_iota(jnp.int32, (8, lanes), 0)
    stats[me] = jnp.where(
        line == 0, laid(top), jnp.where(line == 1, laid(total), jnp.where(line == 2, laid(hit), 0.0))
    )
    sends = [
        push(stats.at[me], stats.at[me], s_send.at[k], s_recv.at[k], at(k)) for k in range(1, peers)
    ]
    for copy in sends:
        copy.start()
    for copy in sends:
        copy.wait_recv()
    every = stats[...]
    best = jnp.max(every[:, 0:1, :], axis=0)
    summed = jnp.sum(every[:, 1:2, :] * jnp.exp(every[:, 0:1, :] - best[None]), axis=0)
    chosen = jnp.sum(every[:, 2:3, :], axis=0)
    used = lax.broadcasted_iota(jnp.int32, (1, lanes), 1) < rows
    logprob = chosen - (best + jnp.log(jnp.where(used, summed, 1.0)))
    out_ref[...] = jnp.broadcast_to(logprob, out_ref.shape)
    for copy in copies + sends:
        copy.wait_send()


def head_call(sizes, own, targets, lm_head):
    ne, nv, nb = sizes
    tokens, width = own.shape
    peers = ne * nv
    dma = pltpu.SemaphoreType.DMA
    vm = pl.BlockSpec(memory_space=pltpu.VMEM)
    return pl.pallas_call(
        functools.partial(head_kernel, ne, nv),
        out_shape=jax.ShapeDtypeStruct((8, 128), jnp.float32),
        in_specs=[vm, vm, pl.BlockSpec(memory_space=pl.ANY)],
        out_specs=vm,
        scratch_shapes=[
            pltpu.VMEM(lm_head.shape, jnp.bfloat16),
            pltpu.VMEM((peers, tokens, width), jnp.bfloat16),
            pltpu.VMEM((peers, 8, 128), jnp.float32),
            dma((4,)),
            dma((2, ne)),
            dma((2, ne)),
            dma((peers,)),
            dma((peers,)),
        ],
        compiler_params=pltpu.CompilerParams(
            collective_id=1, has_side_effects=True, vmem_limit_bytes=VMEM_BYTES - 2 * 1024 * 1024
        ),
        name="head",
    )(own, targets, lm_head)


def kernels_fit(sizes, resid, w_gate, lm_head):
    ne, nv, nb = sizes
    tokens, width = resid.shape[1:]
    hidden_width = w_gate.shape[2]
    rows = ne * nv * nb * tokens
    need = 2 * (3 * width * hidden_width + rows * (3 * width + hidden_width) + 8 * ne * tokens * width)
    group = ne * nv * tokens
    head_need = 2 * (lm_head.shape[0] * width + 4 * group * width)
    return (
        nv == 2
        and nb == 4
        and tokens % 8 == 0
        and width % (128 * COLUMN_CHUNKS) == 0
        and hidden_width % 256 == 0
        and lm_head.shape[0] % 256 == 0
        and group <= 128
        and max(need, head_need) < VMEM_BYTES - 4 * 1024 * 1024
    )


def on_device_kernels(
    sizes,
    resid,
    moe_gain,
    final_gain,
    router,
    w_gate,
    w_up,
    w_down,
    lm_head,
    expert_ids,
    target_ids,
    choice_len,
    choice_question,
):
    ne, nv, nb = sizes
    stream = resid[0].astype(jnp.float32)
    token_count = stream.shape[0]
    normed_in = rms_scale(stream, moe_gain).astype(jnp.bfloat16)
    router_logit = jnp.dot(normed_in, router, preferred_element_type=jnp.float32)
    route_ids = expert_ids[0]
    gate_weights = route_gates(router_logit, route_ids)
    gates = jnp.sum(
        jnp.where(
            route_ids[:, :, None] == jnp.arange(ne, dtype=jnp.int32)[None, None, :],
            gate_weights[:, :, None],
            0.0,
        ),
        axis=1,
    )
    normed_out = experts_call(
        sizes, normed_in, resid[0], gates, final_gain.reshape(1, -1), w_gate, w_up, w_down
    )
    targets = target_ids[0]
    group_tokens = targets.shape[0]
    found = head_call(sizes, normed_out, targets.reshape(-1, 1), lm_head)
    group_logprob = found[0, :group_tokens]
    lengths = choice_len[0]
    positions = jnp.arange(group_tokens, dtype=jnp.int32)
    choice_total = jnp.sum(
        jnp.where(choice_member(lengths, positions), group_logprob[None, :], 0.0), axis=1
    )
    own_first = lax.axis_index(("expert", "vocab")) * token_count
    own_logprob = lax.dynamic_slice_in_dim(group_logprob, own_first, token_count, 0)
    choice_prob = choice_softmax(choice_total, lengths, choice_question[0])
    return (own_logprob.reshape(1, -1), choice_prob.reshape(1, -1))


def either(sizes, *arrays):
    if kernels_fit(sizes, arrays[0], arrays[4], arrays[7]):
        return on_device_kernels(sizes, *arrays)
    return on_device(*arrays)


def solution(mesh):
    sizes = tuple(mesh.shape[axis] for axis in ("expert", "vocab", "batch"))
    return jax.shard_map(
        functools.partial(either, sizes),
        mesh=mesh,
        in_specs=(
            P("batch", ("expert", "vocab"), None),
            P(),
            P(),
            P(),
            P("expert", None, ("vocab", "batch")),
            P("expert", None, ("vocab", "batch")),
            P("expert", ("vocab", "batch"), None),
            P(("expert", "vocab"), None),
            P("batch", ("expert", "vocab"), None),
            P("batch", None),
            P("batch", None),
            P("batch", None),
        ),
        out_specs=(P("batch", ("expert", "vocab")), P("batch", None)),
        check_vma=False,
    )
```
